32 devices in a mesh: prow: 2 (over x), pcol: 16 (over z, y, core).
Axes of the slice: x: 2, y: 2, z: 4, core: 2. Of those that a mesh axis runs over, the one named last changes fastest.
Arguments:
- vectors: float32 [32768, 2048], P('prow', 'pcol'), may hold values from -6 to 6
- reflectors: bfloat16 [4, 256, 32768], P(None, 'pcol', 'prow'), may hold values from -0.03125 to 0.03125
- tau_diag: float32 [4, 256], replicated, may hold values from 0.5 to 1.5
- coupling: float32 [4, 256, 256], replicated, may hold values from -0.375 to 0.375
Outputs:
- result: float32 [32768, 2048], P('prow', 'pcol')
The draws below stay inside these ranges and needn't reach their ends.
All inputs are finite; a program needn't handle non-finite values.
Results may differ from the reference program's by a relative error of at most 0.0003.
Values may be sent and summed in bfloat16 or wider, within the bound.
A program may use at most 128 MiB of HBM per device.

```python
import jax
import jax.numpy as jnp
from jax import lax

N = 32768
NB = 256
PANELS = 4
M = 2048


def steps_of(own_key, extent, pieces, low, top_value):
    def one(dim, parts):
        heights = jax.random.uniform(jax.random.fold_in(jax.random.fold_in(own_key, 6), dim), (parts,), jnp.float32, low / len(pieces), top_value / len(pieces))
        return jnp.repeat(jnp.exp(heights), extent[dim] // parts).reshape((-1,) + (1,) * (len(extent) - dim - 1))

    loudness = one(*pieces[0])
    for cut in pieces[1:]:
        loudness = loudness * one(*cut)
    return loudness


def scatter_about(rng, extent, spread, reach, shards=(), kind=jnp.bfloat16):
    entries = jax.random.normal(rng, extent, jnp.float32) * spread
    if len(shards) > 0:
        entries = steps_of(rng, extent, shards, -0.22, 0.18) * entries
    return jnp.clip(entries, min=-reach, max=reach).astype(kind)


def setup_inputs(seed: int = 0) -> dict:
    streams_of = jax.random.split(jax.random.key(seed), 5)
    return {
        "vectors": scatter_about(streams_of[0], (N, M), 1.0, 6.0, ((0, 2), (1, 16)), jnp.float32),
        "reflectors": scatter_about(streams_of[1], (PANELS, NB, N), N ** -0.5, 0.03125, ((1, 16), (2, 2))),
        "tau_diag": jnp.clip(jax.random.uniform(streams_of[2], (PANELS, NB), jnp.float32, 0.5, 1.5), 0.5, 1.5),
        "coupling": scatter_about(streams_of[3], (PANELS, NB, NB), NB ** -0.5, 0.375, (), jnp.float32),
    }


def reference(vectors, reflectors, tau_diag, coupling):
    current = vectors
    for position in range(PANELS - 1, -1, -1):
        widened = reflectors[position].astype(jnp.float32)
        tri_factor = jnp.diag(tau_diag[position]) + jnp.triu(coupling[position], 1)
        products = jnp.dot(widened, current, precision=lax.Precision.HIGHEST, preferred_element_type=jnp.float32)
        updates = jnp.dot(tri_factor, products, precision=lax.Precision.HIGHEST, preferred_element_type=jnp.float32)
        current = current - jnp.dot(widened.T, updates, precision=lax.Precision.HIGHEST, preferred_element_type=jnp.float32)
    return current
```

```python
import functools

import jax
import jax.numpy as jnp
from jax import lax
from jax.experimental import pallas as pl
from jax.experimental.pallas import tpu as pltpu
from jax.sharding import PartitionSpec as P

MESH = pl.DeviceIdType.MESH
CORES = 2
SIDES = 2


def plain(vectors, reflectors, tau_diag, coupling):
    count = reflectors.shape[0]
    gathered = lax.all_gather(reflectors, "pcol", axis=1, tiled=True)
    current = vectors
    for position in range(count - 1, -1, -1):
        rows_panel = gathered[position]
        widened = rows_panel.astype(jnp.float32)
        tri_factor = jnp.diag(tau_diag[position]) + jnp.triu(coupling[position], 1)
        partial_sum = jnp.dot(
            widened, current, precision=lax.Precision.HIGHEST, preferred_element_type=jnp.float32
        )
        totals = lax.psum(partial_sum, "prow")
        updates = jnp.dot(
            tri_factor, totals, precision=lax.Precision.HIGHEST, preferred_element_type=jnp.float32
        )
        current = current - lax.dot_general(
            widened,
            updates,
            (((0,), (0,)), ((), ())),
            precision=lax.Precision.HIGHEST,
            preferred_element_type=jnp.float32,
        )
    return current


def split(x):
    high = x.astype(jnp.bfloat16)
    low = (x - high.astype(jnp.float32)).astype(jnp.bfloat16)
    return jnp.concatenate([high, low], axis=1)


def joined(x):
    width = x.shape[1] // 2
    return x[:, :width] + x[:, width:]


def kernel(
    length, z_hbm, v_hbm, tau_ref, coup_ref, out_hbm,
    v, z, acc, yhl, wsend, wrecv,
    in_sem, z_sem, out_sem, ring_send, ring_recv, mate_send, mate_recv, w_send, w_recv,
):
    count, own, rows = v_hbm.shape
    cols = z.shape[1]
    nb = v.shape[1]
    half = rows // 2
    deep = length // SIDES
    prow = lax.axis_index("prow")
    pcol = lax.axis_index("pcol")
    core = pcol % CORES
    chip = pcol // CORES
    slow, side = chip // SIDES, chip % SIDES
    place = slow * (1 - 2 * side) + (length - 1) * side

    def pcol_at(position):
        position = (position + length) % length
        on = position // deep
        deep_at = position * (1 - 2 * on) + (length - 1) * on
        return (deep_at * SIDES + on) * CORES + core

    ahead = [pcol_at(place + 1), pcol_at(place - 1)]
    mate = chip * CORES + (1 - core)
    across = 1 - prow

    def shard(k, origin, lo, size):
        start = pl.multiple_of(origin * own, own)
        return v.at[count - 1 - k, pl.ds(start, own), pl.ds(lo, size)]

    far = length // 2
    last = 2 * (far - 1)

    def ring(k, d, t):
        hop = t // 2
        origin = pcol_at(place - hop if d == 0 else place + hop)
        h = d if t == last else t % 2
        ref = shard(k, origin, h * half, half)
        return pltpu.make_async_remote_copy(
            src_ref=ref, dst_ref=ref, send_sem=ring_send.at[k, d, t], recv_sem=ring_recv.at[k, d, t],
            device_id=(prow, ahead[d]), device_id_type=MESH,
        )

    def to_mate(k, j):
        if j == 0:
            origin = pcol
        elif j < far:
            origin = pcol_at(place - j)
        elif j < 2 * far - 1:
            origin = pcol_at(place + (j - far + 1))
        else:
            origin = pcol_at(place + far)
        ref = shard(k, origin, 0, rows)
        return pltpu.make_async_remote_copy(
            src_ref=ref, dst_ref=ref, send_sem=mate_send.at[k, j], recv_sem=mate_recv.at[k, j],
            device_id=(prow, mate), device_id_type=MESH,
        )

    def load(k):
        return pltpu.make_async_copy(
            v_hbm.at[count - 1 - k], shard(k, pcol, 0, rows), in_sem.at[k]
        )

    z_in = pltpu.make_async_copy(z_hbm, z, z_sem)
    for k in range(count):
        load(k).start()
    z_in.start()

    barrier = pltpu.get_barrier_semaphore()
    for target in ((prow, ahead[0]), (prow, ahead[1]), (prow, mate), (across, pcol)):
        pl.semaphore_signal(barrier, inc=1, device_id=target, device_id_type=MESH)
    pl.semaphore_wait(barrier, 4)

    def begin(k):
        load(k).wait()
        for t in range(2):
            for d in range(2):
                ring(k, d, t).start()
        to_mate(k, 0).start()

    def arrived(k, t):
        for d in range(2):
            ring(k, d, t).wait_recv()
            if t + 2 < last or (t + 2 == last and d == 0) or (t + 1 == last and d == 1):
                ring(k, d, min(t + 2, last)).start()
            if t % 2 == 1:
                to_mate(k, (t + 1) // 2 + (far - 1) * d).start()
        if t == last:
            to_mate(k, 2 * far - 1).start()
        if t == last - 1 and k + 1 < count:
            begin(k + 1)

    tile = min(1024, half)
    tiles = rows // tile

    def project(k, lo, hi):
        @pl.loop(lo, hi)
        def _(i):
            at = pl.ds(pl.multiple_of(i * tile, tile), tile)
            acc[...] += jnp.dot(
                v[count - 1 - k, :, at], split(z[at, :]), preferred_element_type=jnp.float32
            )

    def to_across(k):
        return pltpu.make_async_remote_copy(
            src_ref=wsend.at[k], dst_ref=wrecv.at[k], send_sem=w_send.at[k], recv_sem=w_recv.at[k],
            device_id=(across, pcol), device_id_type=MESH,
        )

    def factor(k):
        p = count - 1 - k
        row = lax.broadcasted_iota(jnp.int32, (nb, nb), 0)
        col = lax.broadcasted_iota(jnp.int32, (nb, nb), 1)
        upper = jnp.where(col > row, coup_ref[p], 0.0)
        tri = jnp.where(col == row, tau_ref[p][None, :], upper)
        totals = wsend[k] + wrecv[k]
        y = jnp.dot(tri, totals, precision=lax.Precision.HIGHEST, preferred_element_type=jnp.float32)
        yhl[...] = split(y)

    def out_copy(i):
        at = pl.ds(pl.multiple_of(i * tile, tile), tile)
        return pltpu.make_async_copy(z.at[at, :], out_hbm.at[at, :], out_sem.at[i])

    def update(k, lo, hi):
        @pl.loop(lo, hi)
        def _(i):
            at = pl.ds(pl.multiple_of(i * tile, tile), tile)
            change = lax.dot_general(
                v[count - 1 - k, :, at], yhl[...], (((0,), (0,)), ((), ())),
                preferred_element_type=jnp.float32,
            )
            z[at, :] = z[at, :] - joined(change)
            if k == count - 1:
                out_copy(i).start()

    def compute(k):
        def first():
            for j in range(2 * far):
                to_mate(k, j).wait_recv()
            acc[...] = jnp.zeros_like(acc)
            project(k, 0, tiles // 2)

        def second():
            project(k, tiles // 2, tiles)
            wsend[k] = joined(acc[...])
            to_across(k).start()

        def third():
            to_across(k).wait_recv()
            factor(k)

        quarter = tiles // 4
        return [first, second, third] + [
            functools.partial(update, k, q * quarter, (q + 1) * quarter) for q in range(4)
        ]

    begin(0)
    for k in range(count):
        work = compute(k - 1) if k else [z_in.wait]
        for t in range(last + 1):
            arrived(k, t)
            if t < len(work):
                work[t]()
        for piece in work[last + 1:]:
            piece()
    for piece in compute(count - 1):
        piece()
    for k in range(count):
        for d in range(2):
            for t in range(last + 1):
                ring(k, d, t).wait_send()
        for j in range(2 * far):
            to_mate(k, j).wait_send()
        to_across(k).wait_send()
    for i in range(tiles):
        out_copy(i).wait()


def fused(length, vectors, reflectors, tau_diag, coupling):
    count, own, rows = reflectors.shape
    cols = vectors.shape[1]
    nb = own * length * CORES
    tiles = rows // min(1024, rows // 2)
    messages = length - 1
    vmem = pl.BlockSpec(memory_space=pltpu.VMEM)
    hbm = pl.BlockSpec(memory_space=pl.ANY)
    dma = pltpu.SemaphoreType.DMA
    return pl.pallas_call(
        functools.partial(kernel, length),
        out_shape=jax.ShapeDtypeStruct(vectors.shape, vectors.dtype),
        in_specs=[hbm, hbm, vmem, vmem],
        out_specs=hbm,
        scratch_shapes=[
            pltpu.VMEM((count, nb, rows), reflectors.dtype),
            pltpu.VMEM((rows, cols), jnp.float32),
            pltpu.VMEM((nb, 2 * cols), jnp.float32),
            pltpu.VMEM((nb, 2 * cols), jnp.bfloat16),
            pltpu.VMEM((count, nb, cols), jnp.float32),
            pltpu.VMEM((count, nb, cols), jnp.float32),
            dma((count,)),
            dma,
            dma((tiles,)),
            dma((count, 2, messages)),
            dma((count, 2, messages)),
            dma((count, length)),
            dma((count, length)),
            dma((count,)),
            dma((count,)),
        ],
        compiler_params=pltpu.CompilerParams(
            collective_id=0, has_side_effects=True, vmem_limit_bytes=60 * 1024 * 1024
        ),
    )(vectors, reflectors, tau_diag, coupling)


def on_device(two_rows, length, vectors, reflectors, tau_diag, coupling):
    count, own, rows = reflectors.shape
    cols = vectors.shape[1]
    held = count * own * length * CORES * rows * 2 + rows * cols * 4
    fits = (
        two_rows and length % (2 * SIDES) == 0 and own % 16 == 0 and rows % 4096 == 0
        and cols % 128 == 0 and held <= 48 * 1024 * 1024
    )
    if fits:
        return fused(length, vectors, reflectors, tau_diag, coupling)
    return plain(vectors, reflectors, tau_diag, coupling)


def solution(mesh):
    length = mesh.shape["pcol"] // CORES
    return jax.shard_map(
        functools.partial(on_device, mesh.shape["prow"] == 2, length),
        mesh=mesh,
        in_specs=(P("prow", "pcol"), P(None, "pcol", "prow"), P(), P()),
        out_specs=P("prow", "pcol"),
        check_vma=False,
    )
```

```python
import functools

import jax
import jax.numpy as jnp
from jax import lax
from jax.experimental import pallas as pl
from jax.experimental.pallas import tpu as pltpu
from jax.sharding import PartitionSpec as P

MESH = pl.DeviceIdType.MESH
CORES = 2
SIDES = 2


def plain(vectors, reflectors, tau_diag, coupling):
    count = reflectors.shape[0]
    gathered = lax.all_gather(reflectors, "pcol", axis=1, tiled=True)
    current = vectors
    for position in range(count - 1, -1, -1):
        rows_panel = gathered[position]
        widened = rows_panel.astype(jnp.float32)
        tri_factor = jnp.diag(tau_diag[position]) + jnp.triu(coupling[position], 1)
        partial_sum = jnp.dot(
            widened, current, precision=lax.Precision.HIGHEST, preferred_element_type=jnp.float32
        )
        totals = lax.psum(partial_sum, "prow")
        updates = jnp.dot(
            tri_factor, totals, precision=lax.Precision.HIGHEST, preferred_element_type=jnp.float32
        )
        current = current - lax.dot_general(
            widened,
            updates,
            (((0,), (0,)), ((), ())),
            precision=lax.Precision.HIGHEST,
            preferred_element_type=jnp.float32,
        )
    return current


def split(x):
    high = x.astype(jnp.bfloat16)
    low = (x - high.astype(jnp.float32)).astype(jnp.bfloat16)
    return jnp.concatenate([high, low], axis=1)


def joined(x):
    width = x.shape[1] // 2
    return x[:, :width] + x[:, width:]


def kernel(
    length, z_hbm, v_hbm, tau_hbm, coup_hbm, out_hbm,
    v, z, zhl, acc, tau, tri, nat, yhl, wsend, wrecv,
    in_sem, z_sem, t_sem, out_sem, ring_send, ring_recv, mate_send, mate_recv, w_send, w_recv,
):
    count, own, rows = v_hbm.shape
    nb = v.shape[1]
    group = own * CORES
    half = rows // 2
    deep = length // SIDES
    final = count - 1
    prow = lax.axis_index("prow")
    pcol = lax.axis_index("pcol")
    core = pcol % CORES
    chip = pcol // CORES
    slow, side = chip // SIDES, chip % SIDES
    place = slow * (1 - 2 * side) + (length - 1) * side

    def chip_at(position):
        position = (position + length) % length
        on = position // deep
        return (position * (1 - 2 * on) + (length - 1) * on) * SIDES + on

    ahead = [chip_at(place + 1) * CORES + core, chip_at(place - 1) * CORES + core]
    mate = chip * CORES + (1 - core)
    across = 1 - prow
    far = length // 2
    last = 2 * (far - 1)

    def slot(d, hops):
        return 0 if hops == 0 else min(2 * hops - 1 + d, length - 1)

    def slot_chip(j):
        hops = (j + 1) // 2
        return chip_at(place - hops if j % 2 else place + hops)

    def shard(k, j, lo, size):
        start = pl.multiple_of((j * CORES + core) * own, own)
        return v.at[final - k, pl.ds(start, own), pl.ds(lo, size)]

    def ring(k, d, t):
        hops = t // 2
        h = d if t == last else (t + d) % 2
        return pltpu.make_async_remote_copy(
            src_ref=shard(k, slot(d, hops), h * half, half),
            dst_ref=shard(k, slot(d, hops + 1), h * half, half),
            send_sem=ring_send.at[k, d, t], recv_sem=ring_recv.at[k, d, t],
            device_id=(prow, ahead[d]), device_id_type=MESH,
        )

    def to_mate(k, j):
        ref = shard(k, j, 0, rows)
        return pltpu.make_async_remote_copy(
            src_ref=ref, dst_ref=ref, send_sem=mate_send.at[k, j], recv_sem=mate_recv.at[k, j],
            device_id=(prow, mate), device_id_type=MESH,
        )

    def load(k):
        return pltpu.make_async_copy(v_hbm.at[final - k], shard(k, 0, 0, rows), in_sem.at[k])

    load(0).start()
    barrier = pltpu.get_barrier_semaphore()
    for target in ((prow, ahead[0]), (prow, ahead[1]), (prow, mate), (across, pcol)):
        pl.semaphore_signal(barrier, inc=1, device_id=target, device_id_type=MESH)
    pl.semaphore_wait(barrier, 4)

    def begin(k):
        load(k).wait()
        for t in range(2):
            for d in range(2):
                ring(k, d, t).start()
        to_mate(k, 0).start()

    def arrived(k, t):
        for d in range(2):
            ring(k, d, t).wait_recv()
            if t + 2 <= last:
                ring(k, d, t + 2).start()
            if t % 2 == 1:
                to_mate(k, slot(d, (t + 1) // 2)).start()
        if t == last:
            to_mate(k, length - 1).start()
        if t == last - 2 and k < final:
            begin(k + 1)

    tile = min(1024, half)
    tiles = rows // tile

    def tile_at(i):
        return pl.ds(pl.multiple_of(i * tile, tile), tile)

    def project(k, lo, hi, first=0, beyond=nb):
        @pl.loop(lo, hi)
        def _(i):
            at = tile_at(i)
            acc[first:beyond, :] += jnp.dot(
                v[final - k, first:beyond, at], zhl[at, :], preferred_element_type=jnp.float32
            )

    cuts = [0, (length - 3) * group, (length - 1) * group, nb]

    def to_across(k, part=None):
        sem = k if part is None else final + part
        at = pl.ds(0, nb) if part is None else pl.ds(cuts[part], cuts[part + 1] - cuts[part])
        return pltpu.make_async_remote_copy(
            src_ref=wsend.at[k, at], dst_ref=wrecv.at[k, at], send_sem=w_send.at[sem], recv_sem=w_recv.at[sem],
            device_id=(across, pcol), device_id_type=MESH,
        )

    def mates(k, lo, hi):
        for j in range(lo, hi):
            to_mate(k, j).wait_recv()

    def factor(k):
        for j in range(length):
            mine = pl.ds(j * group, group)
            at = pl.ds(pl.multiple_of(slot_chip(j) * group, group), group)
            nat[at, :] = wsend[k, mine, :] + wrecv[k, mine, :]
        nat[...] = jnp.dot(
            tri[final - k], nat[...], precision=lax.Precision.HIGHEST, preferred_element_type=jnp.float32
        )
        for j in range(length):
            at = pl.ds(pl.multiple_of(slot_chip(j) * group, group), group)
            yhl[j * group:(j + 1) * group, :] = split(nat[at, :])

    def out_copy(i):
        at = tile_at(i)
        return pltpu.make_async_copy(z.at[at, :], out_hbm.at[at, :], out_sem.at[i])

    def update(k, lo, hi):
        @pl.loop(lo, hi)
        def _(i):
            at = tile_at(i)
            change = lax.dot_general(
                v[final - k, :, at], yhl[...], (((0,), (0,)), ((), ())),
                preferred_element_type=jnp.float32,
            )
            fresh = z[at, :] - joined(change)
            z[at, :] = fresh
            if k < final:
                zhl[at, :] = split(fresh)
            else:
                out_copy(i).start()

    def clear():
        acc[...] = jnp.zeros_like(acc)

    def head(k):
        mates(k, 0, length)
        clear()
        project(k, 0, tiles // 2)

    def rest(k):
        project(k, tiles // 2, tiles)
        wsend[k] = joined(acc[...])
        to_across(k).start()

    def solve(k):
        to_across(k).wait_recv()
        factor(k)

    def quarters(k):
        return [
            functools.partial(update, k, q * tiles // 4, (q + 1) * tiles // 4) for q in range(4)
        ]

    def finish(part):
        slots = [cuts[part] // group, cuts[part + 1] // group]
        mates(final, *slots)
        project(final, 0, tiles, cuts[part], cuts[part + 1])
        wsend[final, cuts[part]:cuts[part + 1], :] = joined(acc[cuts[part]:cuts[part + 1], :])
        to_across(final, part).start()

    def opening():
        z_in.wait()
        tau_in.wait()
        coup_in.wait()

        @pl.loop(0, tiles)
        def _(i):
            at = tile_at(i)
            zhl[at, :] = split(z[at, :])

    def triangles():
        row = lax.broadcasted_iota(jnp.int32, (nb, nb), 0)
        col = lax.broadcasted_iota(jnp.int32, (nb, nb), 1)
        for p in range(count):
            upper = jnp.where(col > row, tri[p], 0.0)
            tri[p] = jnp.where(col == row, tau[p][None, :], upper)

    begin(0)
    z_in = pltpu.make_async_copy(z_hbm, z, z_sem)
    tau_in = pltpu.make_async_copy(tau_hbm, tau, t_sem.at[0])
    coup_in = pltpu.make_async_copy(coup_hbm, tri, t_sem.at[1])
    for k in range(1, count):
        load(k).start()
    z_in.start()
    tau_in.start()
    coup_in.start()
    for k in range(count):
        if k == 0:
            work = [[opening], [triangles]]
        else:
            q = quarters(k - 1)
            a, b, c = [functools.partial(f, k - 1) for f in (head, rest, solve)]
            work = [[a], [b], [c]] + [[piece] for piece in q]
            if k == final:
                work = [[a], [b], [c, q[0]], [q[1], q[2]], [q[3], clear, functools.partial(finish, 0)]]
                work.append([functools.partial(finish, 1)])
        for t in range(last + 1):
            arrived(k, t)
            for piece in work[t] if t < len(work) else []:
                piece()
        for pieces in work[last + 1:]:
            for piece in pieces:
                piece()
    finish(2)
    for part in range(3):
        to_across(final, part).wait_recv()
    factor(final)
    update(final, 0, tiles)
    for k in range(count):
        for d in range(2):
            for t in range(last + 1):
                ring(k, d, t).wait_send()
        for j in range(length):
            to_mate(k, j).wait_send()
        if k < final:
            to_across(k).wait_send()
    for part in range(3):
        to_across(final, part).wait_send()
    for i in range(tiles):
        out_copy(i).wait()


def fused(length, vectors, reflectors, tau_diag, coupling):
    count, own, rows = reflectors.shape
    cols = vectors.shape[1]
    nb = own * length * CORES
    tiles = rows // min(1024, rows // 2)
    messages = length - 1
    hbm = pl.BlockSpec(memory_space=pl.ANY)
    dma = pltpu.SemaphoreType.DMA
    return pl.pallas_call(
        functools.partial(kernel, length),
        out_shape=jax.ShapeDtypeStruct(vectors.shape, vectors.dtype),
        in_specs=[hbm] * 4,
        out_specs=hbm,
        scratch_shapes=[
            pltpu.VMEM((count, nb, rows), reflectors.dtype),
            pltpu.VMEM((rows, cols), jnp.float32),
            pltpu.VMEM((rows, 2 * cols), jnp.bfloat16),
            pltpu.VMEM((nb, 2 * cols), jnp.float32),
            pltpu.VMEM((count, nb), jnp.float32),
            pltpu.VMEM((count, nb, nb), jnp.float32),
            pltpu.VMEM((nb, cols), jnp.float32),
            pltpu.VMEM((nb, 2 * cols), jnp.bfloat16),
            pltpu.VMEM((count, nb, cols), jnp.float32),
            pltpu.VMEM((count, nb, cols), jnp.float32),
            dma((count,)),
            dma,
            dma((2,)),
            dma((tiles,)),
            dma((count, 2, messages)),
            dma((count, 2, messages)),
            dma((count, length)),
            dma((count, length)),
            dma((count + 2,)),
            dma((count + 2,)),
        ],
        compiler_params=pltpu.CompilerParams(
            collective_id=0, has_side_effects=True, vmem_limit_bytes=60 * 1024 * 1024
        ),
    )(vectors, reflectors, tau_diag, coupling)


def on_device(two_rows, length, vectors, reflectors, tau_diag, coupling):
    count, own, rows = reflectors.shape
    cols = vectors.shape[1]
    held = count * own * length * CORES * rows * 2 + rows * cols * 8
    fits = (
        two_rows and length % (2 * SIDES) == 0 and length >= 8 and count >= 2 and own % 16 == 0 and rows % 4096 == 0
        and cols % 128 == 0 and held <= 52 * 1024 * 1024
    )
    if fits:
        return fused(length, vectors, reflectors, tau_diag, coupling)
    return plain(vectors, reflectors, tau_diag, coupling)


def solution(mesh):
    length = mesh.shape["pcol"] // CORES
    return jax.shard_map(
        functools.partial(on_device, mesh.shape["prow"] == 2, length),
        mesh=mesh,
        in_specs=(P("prow", "pcol"), P(None, "pcol", "prow"), P(), P()),
        out_specs=P("prow", "pcol"),
        check_vma=False,
    )
```

```python
import functools

import jax
import jax.numpy as jnp
from jax import lax
from jax.experimental import pallas as pl
from jax.experimental.pallas import tpu as pltpu
from jax.sharding import PartitionSpec as P

MESH = pl.DeviceIdType.MESH
CORES = 2
SIDES = 2


def plain(vectors, reflectors, tau_diag, coupling):
    count = reflectors.shape[0]
    gathered = lax.all_gather(reflectors, "pcol", axis=1, tiled=True)
    current = vectors
    for position in range(count - 1, -1, -1):
        rows_panel = gathered[position]
        widened = rows_panel.astype(jnp.float32)
        tri_factor = jnp.diag(tau_diag[position]) + jnp.triu(coupling[position], 1)
        partial_sum = jnp.dot(
            widened, current, precision=lax.Precision.HIGHEST, preferred_element_type=jnp.float32
        )
        totals = lax.psum(partial_sum, "prow")
        updates = jnp.dot(
            tri_factor, totals, precision=lax.Precision.HIGHEST, preferred_element_type=jnp.float32
        )
        current = current - lax.dot_general(
            widened,
            updates,
            (((0,), (0,)), ((), ())),
            precision=lax.Precision.HIGHEST,
            preferred_element_type=jnp.float32,
        )
    return current


def split(x):
    high = x.astype(jnp.bfloat16)
    low = (x - high.astype(jnp.float32)).astype(jnp.bfloat16)
    return jnp.concatenate([high, low], axis=1)


def joined(x):
    width = x.shape[1] // 2
    return x[:, :width] + x[:, width:]


def kernel(
    length, z_hbm, v_hbm, tau_hbm, coup_hbm, z,
    v, zhl, acc, tau, tri, nat, yhl, wsend, wrecv,
    in_sem, z_sem, t_sem, ring_send, ring_recv, mate_send, mate_recv, w_send, w_recv,
):
    count, own, rows = v_hbm.shape
    nb = v.shape[1]
    group = own * CORES
    half = rows // 2
    deep = length // SIDES
    final = count - 1
    prow = lax.axis_index("prow")
    pcol = lax.axis_index("pcol")
    core = pcol % CORES
    chip = pcol // CORES
    slow, side = chip // SIDES, chip % SIDES
    place = slow * (1 - 2 * side) + (length - 1) * side

    def chip_at(position):
        position = (position + length) % length
        on = position // deep
        return (position * (1 - 2 * on) + (length - 1) * on) * SIDES + on

    ahead = [chip_at(place + 1) * CORES + core, chip_at(place - 1) * CORES + core]
    mate = chip * CORES + (1 - core)
    across = 1 - prow
    far = length // 2
    last = 2 * (far - 1)

    def slot(d, hops):
        return 0 if hops == 0 else min(2 * hops - 1 + d, length - 1)

    def slot_chip(j):
        hops = (j + 1) // 2
        return chip_at(place - hops if j % 2 else place + hops)

    def shard(k, j, lo, size):
        start = pl.multiple_of((j * CORES + core) * own, own)
        return v.at[final - k, pl.ds(start, own), pl.ds(lo, size)]

    def ring(k, d, t):
        hops = t // 2
        h = d if t == last else (t + d) % 2
        return pltpu.make_async_remote_copy(
            src_ref=shard(k, slot(d, hops), h * half, half),
            dst_ref=shard(k, slot(d, hops + 1), h * half, half),
            send_sem=ring_send.at[k, d, t], recv_sem=ring_recv.at[k, d, t],
            device_id=(prow, ahead[d]), device_id_type=MESH,
        )

    def to_mate(k, j):
        ref = shard(k, j, 0, rows)
        return pltpu.make_async_remote_copy(
            src_ref=ref, dst_ref=ref, send_sem=mate_send.at[k, j], recv_sem=mate_recv.at[k, j],
            device_id=(prow, mate), device_id_type=MESH,
        )

    def load(k):
        return pltpu.make_async_copy(v_hbm.at[final - k], shard(k, 0, 0, rows), in_sem.at[k])

    load(0).start()
    barrier = pltpu.get_barrier_semaphore()
    for target in ((prow, ahead[0]), (prow, ahead[1]), (prow, mate), (across, pcol)):
        pl.semaphore_signal(barrier, inc=1, device_id=target, device_id_type=MESH)
    pl.semaphore_wait(barrier, 4)

    def begin(k):
        load(k).wait()
        for t in range(2):
            for d in range(2):
                ring(k, d, t).start()
        to_mate(k, 0).start()

    def arrived(k, t):
        for d in range(2):
            ring(k, d, t).wait_recv()
            if t + 2 <= last:
                ring(k, d, t + 2).start()
            if t % 2 == 1:
                to_mate(k, slot(d, (t + 1) // 2)).start()
        if t == last:
            to_mate(k, length - 1).start()
        if t == last - 2 and k < final:
            begin(k + 1)

    tile = min(1024, half)
    tiles = rows // tile

    def tile_at(i):
        return pl.ds(pl.multiple_of(i * tile, tile), tile)

    def project(k, lo, hi, first=0, beyond=nb):
        @pl.loop(lo, hi)
        def _(i):
            at = tile_at(i)
            acc[first:beyond, :] += jnp.dot(
                v[final - k, first:beyond, at], zhl[at, :], preferred_element_type=jnp.float32
            )

    cuts = [0, (length - 3) * group, (length - 1) * group, nb]

    def to_across(k, part=None):
        sem = k if part is None else final + part
        at = pl.ds(0, nb) if part is None else pl.ds(cuts[part], cuts[part + 1] - cuts[part])
        return pltpu.make_async_remote_copy(
            src_ref=wsend.at[k, at], dst_ref=wrecv.at[k, at], send_sem=w_send.at[sem], recv_sem=w_recv.at[sem],
            device_id=(across, pcol), device_id_type=MESH,
        )

    def mates(k, lo, hi):
        for j in range(lo, hi):
            to_mate(k, j).wait_recv()

    def factor(k):
        for j in range(length):
            mine = pl.ds(j * group, group)
            at = pl.ds(pl.multiple_of(slot_chip(j) * group, group), group)
            nat[at, :] = wsend[k, mine, :] + wrecv[k, mine, :]
        nat[...] = jnp.dot(
            tri[final - k], nat[...], precision=lax.Precision.HIGHEST, preferred_element_type=jnp.float32
        )
        for j in range(length):
            at = pl.ds(pl.multiple_of(slot_chip(j) * group, group), group)
            yhl[j * group:(j + 1) * group, :] = split(nat[at, :])

    def update(k, lo, hi):
        @pl.loop(lo, hi)
        def _(i):
            at = tile_at(i)
            change = lax.dot_general(
                v[final - k, :, at], yhl[...], (((0,), (0,)), ((), ())),
                preferred_element_type=jnp.float32,
            )
            fresh = z[at, :] - joined(change)
            z[at, :] = fresh
            if k < final:
                zhl[at, :] = split(fresh)

    def clear():
        acc[...] = jnp.zeros_like(acc)

    def head(k):
        mates(k, 0, length)
        clear()
        project(k, 0, tiles // 2)

    def rest(k):
        project(k, tiles // 2, tiles)
        wsend[k] = joined(acc[...])
        to_across(k).start()

    def solve(k):
        to_across(k).wait_recv()
        factor(k)

    def quarters(k):
        return [
            functools.partial(update, k, q * tiles // 4, (q + 1) * tiles // 4) for q in range(4)
        ]

    def finish(part):
        slots = [cuts[part] // group, cuts[part + 1] // group]
        mates(final, *slots)
        project(final, 0, tiles, cuts[part], cuts[part + 1])
        wsend[final, cuts[part]:cuts[part + 1], :] = joined(acc[cuts[part]:cuts[part + 1], :])
        to_across(final, part).start()

    def opening():
        z_in.wait()
        tau_in.wait()
        coup_in.wait()

        @pl.loop(0, tiles)
        def _(i):
            at = tile_at(i)
            zhl[at, :] = split(z[at, :])

    def triangles():
        row = lax.broadcasted_iota(jnp.int32, (nb, nb), 0)
        col = lax.broadcasted_iota(jnp.int32, (nb, nb), 1)
        for p in range(count):
            upper = jnp.where(col > row, tri[p], 0.0)
            tri[p] = jnp.where(col == row, tau[p][None, :], upper)

    begin(0)
    z_in = pltpu.make_async_copy(z_hbm, z, z_sem)
    tau_in = pltpu.make_async_copy(tau_hbm, tau, t_sem.at[0])
    coup_in = pltpu.make_async_copy(coup_hbm, tri, t_sem.at[1])
    for k in range(1, count):
        load(k).start()
    z_in.start()
    tau_in.start()
    coup_in.start()
    for k in range(count):
        if k == 0:
            work = [[opening], [triangles]]
        else:
            q = quarters(k - 1)
            a, b, c = [functools.partial(f, k - 1) for f in (head, rest, solve)]
            work = [[a], [b], [c]] + [[piece] for piece in q]
            if k == final:
                work = [[a], [b], [c, q[0]], [q[1], q[2]], [q[3], clear, functools.partial(finish, 0)]]
                work.append([functools.partial(finish, 1)])
        for t in range(last + 1):
            arrived(k, t)
            for piece in work[t] if t < len(work) else []:
                piece()
        for pieces in work[last + 1:]:
            for piece in pieces:
                piece()
    finish(2)
    for part in range(3):
        to_across(final, part).wait_recv()
    factor(final)
    update(final, 0, tiles)
    for k in range(count):
        for d in range(2):
            for t in range(last + 1):
                ring(k, d, t).wait_send()
        for j in range(length):
            to_mate(k, j).wait_send()
        if k < final:
            to_across(k).wait_send()
    for part in range(3):
        to_across(final, part).wait_send()


def fused(length, vectors, reflectors, tau_diag, coupling):
    count, own, rows = reflectors.shape
    cols = vectors.shape[1]
    nb = own * length * CORES
    messages = length - 1
    hbm = pl.BlockSpec(memory_space=pl.ANY)
    dma = pltpu.SemaphoreType.DMA
    return pl.pallas_call(
        functools.partial(kernel, length),
        out_shape=pltpu.VMEM(vectors.shape, vectors.dtype),
        in_specs=[hbm] * 4,
        out_specs=pl.BlockSpec(memory_space=pltpu.VMEM),
        scratch_shapes=[
            pltpu.VMEM((count, nb, rows), reflectors.dtype),
            pltpu.VMEM((rows, 2 * cols), jnp.bfloat16),
            pltpu.VMEM((nb, 2 * cols), jnp.float32),
            pltpu.VMEM((count, nb), jnp.float32),
            pltpu.VMEM((count, nb, nb), jnp.float32),
            pltpu.VMEM((nb, cols), jnp.float32),
            pltpu.VMEM((nb, 2 * cols), jnp.bfloat16),
            pltpu.VMEM((count, nb, cols), jnp.float32),
            pltpu.VMEM((count, nb, cols), jnp.float32),
            dma((count,)),
            dma,
            dma((2,)),
            dma((count, 2, messages)),
            dma((count, 2, messages)),
            dma((count, length)),
            dma((count, length)),
            dma((count + 2,)),
            dma((count + 2,)),
        ],
        compiler_params=pltpu.CompilerParams(
            collective_id=0, has_side_effects=True, vmem_limit_bytes=48 * 1024 * 1024
        ),
    )(vectors, reflectors, tau_diag, coupling)


def on_device(two_rows, length, vectors, reflectors, tau_diag, coupling):
    count, own, rows = reflectors.shape
    cols = vectors.shape[1]
    held = count * own * length * CORES * rows * 2 + rows * cols * 8
    fits = (
        two_rows and length % (2 * SIDES) == 0 and length >= 8 and count >= 2 and own % 16 == 0 and rows % 4096 == 0
        and cols % 128 == 0 and held <= 52 * 1024 * 1024
    )
    if fits:
        return fused(length, vectors, reflectors, tau_diag, coupling)
    return plain(vectors, reflectors, tau_diag, coupling)


def solution(mesh):
    length = mesh.shape["pcol"] // CORES
    return jax.shard_map(
        functools.partial(on_device, mesh.shape["prow"] == 2, length),
        mesh=mesh,
        in_specs=(P("prow", "pcol"), P(None, "pcol", "prow"), P(), P()),
        out_specs=P("prow", "pcol"),
        check_vma=False,
    )
```

```python
import functools

import jax
import jax.numpy as jnp
from jax import lax
from jax.experimental import pallas as pl
from jax.experimental.pallas import tpu as pltpu
from jax.sharding import PartitionSpec as P

MESH = pl.DeviceIdType.MESH
CORES = 2
SIDES = 2


def plain(vectors, reflectors, tau_diag, coupling):
    count = reflectors.shape[0]
    gathered = lax.all_gather(reflectors, "pcol", axis=1, tiled=True)
    current = vectors
    for position in range(count - 1, -1, -1):
        rows_panel = gathered[position]
        widened = rows_panel.astype(jnp.float32)
        tri_factor = jnp.diag(tau_diag[position]) + jnp.triu(coupling[position], 1)
        partial_sum = jnp.dot(
            widened, current, precision=lax.Precision.HIGHEST, preferred_element_type=jnp.float32
        )
        totals = lax.psum(partial_sum, "prow")
        updates = jnp.dot(
            tri_factor, totals, precision=lax.Precision.HIGHEST, preferred_element_type=jnp.float32
        )
        current = current - lax.dot_general(
            widened,
            updates,
            (((0,), (0,)), ((), ())),
            precision=lax.Precision.HIGHEST,
            preferred_element_type=jnp.float32,
        )
    return current


def split(x):
    high = x.astype(jnp.bfloat16)
    low = (x - high.astype(jnp.float32)).astype(jnp.bfloat16)
    return jnp.concatenate([high, low], axis=1)


def joined(x):
    width = x.shape[1] // 2
    return x[:, :width] + x[:, width:]


def kernel(
    length, z_hbm, v_hbm, tau_hbm, coup_hbm, z, ending, yhl,
    v, zhl, acc, tau, tri, nat, wsend, wrecv,
    in_sem, z_sem, t_sem, ring_send, ring_recv, mate_send, mate_recv, w_send, w_recv,
):
    count, own, rows = v_hbm.shape
    nb = ending.shape[0]
    group = own * CORES
    half = rows // 2
    deep = length // SIDES
    final = count - 1
    prow = lax.axis_index("prow")
    pcol = lax.axis_index("pcol")
    core = pcol % CORES
    chip = pcol // CORES
    slow, side = chip // SIDES, chip % SIDES
    place = slow * (1 - 2 * side) + (length - 1) * side

    def chip_at(position):
        position = (position + length) % length
        on = position // deep
        return (position * (1 - 2 * on) + (length - 1) * on) * SIDES + on

    ahead = [chip_at(place + 1) * CORES + core, chip_at(place - 1) * CORES + core]
    mate = chip * CORES + (1 - core)
    across = 1 - prow
    far = length // 2
    last = 2 * (far - 1)

    def slot(d, hops):
        return 0 if hops == 0 else min(2 * hops - 1 + d, length - 1)

    def slot_chip(j):
        hops = (j + 1) // 2
        return chip_at(place - hops if j % 2 else place + hops)

    def shard(k, j, lo, size):
        start = pl.multiple_of((j * CORES + core) * own, own)
        at = (pl.ds(start, own), pl.ds(lo, size))
        return ending.at[at] if k == final else v.at[(k,) + at]

    def ring(k, d, t):
        hops = t // 2
        h = d if t == last else (t + d) % 2
        return pltpu.make_async_remote_copy(
            src_ref=shard(k, slot(d, hops), h * half, half),
            dst_ref=shard(k, slot(d, hops + 1), h * half, half),
            send_sem=ring_send.at[k, d, t], recv_sem=ring_recv.at[k, d, t],
            device_id=(prow, ahead[d]), device_id_type=MESH,
        )

    def to_mate(k, j):
        ref = shard(k, j, 0, rows)
        return pltpu.make_async_remote_copy(
            src_ref=ref, dst_ref=ref, send_sem=mate_send.at[k, j], recv_sem=mate_recv.at[k, j],
            device_id=(prow, mate), device_id_type=MESH,
        )

    def load(k):
        return pltpu.make_async_copy(v_hbm.at[final - k], shard(k, 0, 0, rows), in_sem.at[k])

    load(0).start()
    barrier = pltpu.get_barrier_semaphore()
    for target in ((prow, ahead[0]), (prow, ahead[1]), (prow, mate), (across, pcol)):
        pl.semaphore_signal(barrier, inc=1, device_id=target, device_id_type=MESH)
    pl.semaphore_wait(barrier, 4)

    def begin(k):
        load(k).wait()
        for t in range(2):
            for d in range(2):
                ring(k, d, t).start()
        to_mate(k, 0).start()

    def arrived(k, t):
        for d in range(2):
            ring(k, d, t).wait_recv()
            if t + 2 <= last:
                ring(k, d, t + 2).start()
            if t % 2 == 1:
                to_mate(k, slot(d, (t + 1) // 2)).start()
        if t == last:
            to_mate(k, length - 1).start()
        if t == last - 2 and k < final:
            begin(k + 1)

    tile = min(1024, half)
    tiles = rows // tile

    def tile_at(i):
        return pl.ds(pl.multiple_of(i * tile, tile), tile)

    def panel(k):
        return ending if k == final else v.at[k]

    def project(k, lo, hi, first=0, beyond=nb):
        @pl.loop(lo, hi)
        def _(i):
            at = tile_at(i)
            acc[first:beyond, :] += jnp.dot(
                panel(k)[first:beyond, at], zhl[at, :], preferred_element_type=jnp.float32
            )

    cuts = [0, (length - 3) * group, (length - 1) * group, nb]

    def to_across(k, part=None):
        sem = k if part is None else final + part
        at = pl.ds(0, nb) if part is None else pl.ds(cuts[part], cuts[part + 1] - cuts[part])
        return pltpu.make_async_remote_copy(
            src_ref=wsend.at[k, at], dst_ref=wrecv.at[k, at], send_sem=w_send.at[sem], recv_sem=w_recv.at[sem],
            device_id=(across, pcol), device_id_type=MESH,
        )

    def mates(k, lo, hi):
        for j in range(lo, hi):
            to_mate(k, j).wait_recv()

    def factor(k):
        for j in range(length):
            mine = pl.ds(j * group, group)
            at = pl.ds(pl.multiple_of(slot_chip(j) * group, group), group)
            nat[at, :] = wsend[k, mine, :] + wrecv[k, mine, :]
        nat[...] = jnp.dot(
            tri[final - k], nat[...], precision=lax.Precision.HIGHEST, preferred_element_type=jnp.float32
        )
        for j in range(length):
            at = pl.ds(pl.multiple_of(slot_chip(j) * group, group), group)
            yhl[j * group:(j + 1) * group, :] = split(nat[at, :])

    def update(k, lo, hi):
        @pl.loop(lo, hi)
        def _(i):
            at = tile_at(i)
            change = lax.dot_general(
                panel(k)[:, at], yhl[...], (((0,), (0,)), ((), ())),
                preferred_element_type=jnp.float32,
            )
            fresh = z[at, :] - joined(change)
            z[at, :] = fresh
            zhl[at, :] = split(fresh)

    def clear():
        acc[...] = jnp.zeros_like(acc)

    def head(k):
        mates(k, 0, length)
        clear()
        project(k, 0, tiles // 2)

    def rest(k):
        project(k, tiles // 2, tiles)
        wsend[k] = joined(acc[...])
        to_across(k).start()

    def solve(k):
        to_across(k).wait_recv()
        factor(k)

    def quarters(k):
        return [
            functools.partial(update, k, q * tiles // 4, (q + 1) * tiles // 4) for q in range(4)
        ]

    def finish(part):
        slots = [cuts[part] // group, cuts[part + 1] // group]
        mates(final, *slots)
        project(final, 0, tiles, cuts[part], cuts[part + 1])
        wsend[final, cuts[part]:cuts[part + 1], :] = joined(acc[cuts[part]:cuts[part + 1], :])
        to_across(final, part).start()

    def opening():
        z_in.wait()
        tau_in.wait()
        coup_in.wait()

        @pl.loop(0, tiles)
        def _(i):
            at = tile_at(i)
            zhl[at, :] = split(z[at, :])

    def triangles():
        row = lax.broadcasted_iota(jnp.int32, (nb, nb), 0)
        col = lax.broadcasted_iota(jnp.int32, (nb, nb), 1)
        for p in range(count):
            upper = jnp.where(col > row, tri[p], 0.0)
            tri[p] = jnp.where(col == row, tau[p][None, :], upper)

    begin(0)
    z_in = pltpu.make_async_copy(z_hbm, z, z_sem)
    tau_in = pltpu.make_async_copy(tau_hbm, tau, t_sem.at[0])
    coup_in = pltpu.make_async_copy(coup_hbm, tri, t_sem.at[1])
    for k in range(1, count):
        load(k).start()
    z_in.start()
    tau_in.start()
    coup_in.start()
    for k in range(count):
        if k == 0:
            work = [[opening], [triangles]]
        else:
            q = quarters(k - 1)
            a, b, c = [functools.partial(f, k - 1) for f in (head, rest, solve)]
            work = [[a], [b], [c]] + [[piece] for piece in q]
            if k == final:
                work = [[a], [b], [c, q[0]], [q[1], q[2]], [q[3], clear, functools.partial(finish, 0)]]
                work.append([functools.partial(finish, 1)])
        for t in range(last + 1):
            arrived(k, t)
            for piece in work[t] if t < len(work) else []:
                piece()
        for pieces in work[last + 1:]:
            for piece in pieces:
                piece()
    finish(2)
    for part in range(3):
        to_across(final, part).wait_recv()
    factor(final)
    for k in range(count):
        for d in range(2):
            for t in range(last + 1):
                ring(k, d, t).wait_send()
        for j in range(length):
            to_mate(k, j).wait_send()
        if k < final:
            to_across(k).wait_send()
    for part in range(3):
        to_across(final, part).wait_send()


def closing(z, panel, yhl, out_hbm, fresh, out_sem):
    tiles = out_sem.shape[0]
    tile = z.shape[0] // tiles

    def out_copy(i):
        at = pl.ds(pl.multiple_of(i * tile, tile), tile)
        return pltpu.make_async_copy(fresh.at[at, :], out_hbm.at[at, :], out_sem.at[i])

    @pl.loop(0, tiles)
    def _(i):
        at = pl.ds(pl.multiple_of(i * tile, tile), tile)
        change = lax.dot_general(
            panel[:, at], yhl[...], (((0,), (0,)), ((), ())), preferred_element_type=jnp.float32
        )
        fresh[at, :] = z[at, :] - joined(change)
        out_copy(i).start()

    @pl.loop(0, tiles)
    def _(i):
        out_copy(i).wait()


def fused(length, vectors, reflectors, tau_diag, coupling):
    count, own, rows = reflectors.shape
    cols = vectors.shape[1]
    nb = own * length * CORES
    messages = length - 1
    hbm = pl.BlockSpec(memory_space=pl.ANY)
    vmem = pl.BlockSpec(memory_space=pltpu.VMEM)
    dma = pltpu.SemaphoreType.DMA
    current, panel, updates = pl.pallas_call(
        functools.partial(kernel, length),
        out_shape=[
            pltpu.VMEM(vectors.shape, vectors.dtype),
            pltpu.VMEM((nb, rows), reflectors.dtype),
            pltpu.VMEM((nb, 2 * cols), jnp.bfloat16),
        ],
        in_specs=[hbm] * 4,
        out_specs=[vmem] * 3,
        scratch_shapes=[
            pltpu.VMEM((count - 1, nb, rows), reflectors.dtype),
            pltpu.VMEM((rows, 2 * cols), jnp.bfloat16),
            pltpu.VMEM((nb, 2 * cols), jnp.float32),
            pltpu.VMEM((count, nb), jnp.float32),
            pltpu.VMEM((count, nb, nb), jnp.float32),
            pltpu.VMEM((nb, cols), jnp.float32),
            pltpu.VMEM((count, nb, cols), jnp.float32),
            pltpu.VMEM((count, nb, cols), jnp.float32),
            dma((count,)),
            dma,
            dma((2,)),
            dma((count, 2, messages)),
            dma((count, 2, messages)),
            dma((count, length)),
            dma((count, length)),
            dma((count + 2,)),
            dma((count + 2,)),
        ],
        compiler_params=pltpu.CompilerParams(
            collective_id=0, has_side_effects=True, vmem_limit_bytes=40 * 1024 * 1024
        ),
    )(vectors, reflectors, tau_diag, coupling)
    tiles = rows // min(1024, rows // 2)
    return pl.pallas_call(
        closing,
        out_shape=jax.ShapeDtypeStruct(vectors.shape, vectors.dtype),
        in_specs=[vmem] * 3,
        out_specs=hbm,
        scratch_shapes=[pltpu.VMEM(vectors.shape, jnp.float32), dma((tiles,))],
        compiler_params=pltpu.CompilerParams(vmem_limit_bytes=16 * 1024 * 1024),
    )(current, panel, updates)


def on_device(two_rows, length, vectors, reflectors, tau_diag, coupling):
    count, own, rows = reflectors.shape
    cols = vectors.shape[1]
    held = count * own * length * CORES * rows * 2 + rows * cols * 8
    fits = (
        two_rows and length % (2 * SIDES) == 0 and length >= 8 and count >= 2 and own % 16 == 0 and rows % 4096 == 0
        and cols % 128 == 0 and held <= 52 * 1024 * 1024
    )
    if fits:
        return fused(length, vectors, reflectors, tau_diag, coupling)
    return plain(vectors, reflectors, tau_diag, coupling)


def solution(mesh):
    length = mesh.shape["pcol"] // CORES
    return jax.shard_map(
        functools.partial(on_device, mesh.shape["prow"] == 2, length),
        mesh=mesh,
        in_specs=(P("prow", "pcol"), P(None, "pcol", "prow"), P(), P()),
        out_specs=P("prow", "pcol"),
        check_vma=False,
    )
```
